32 devices in a mesh: row: 16 (over z, y, core), col: 2 (over x).
Axes of the slice: x: 2, y: 2, z: 4, core: 2. Of those that a mesh axis runs over, the one named last changes fastest.
Arguments:
- pair_act: bfloat16 [192, 192, 128], P('row', 'col'), may hold values from -6 to 6
- tile_mask: int32 [12, 12], replicated, may hold values 0 or 1
- w_left_gate: bfloat16 [128, 128], replicated, may hold values from -0.5 to 0.5
- w_left: bfloat16 [128, 128], replicated, may hold values from -0.5 to 0.5
- w_right_gate: bfloat16 [128, 128], replicated, may hold values from -0.5 to 0.5
- w_right: bfloat16 [128, 128], replicated, may hold values from -0.5 to 0.5
- w_out_gate: bfloat16 [128, 128], replicated, may hold values from -0.5 to 0.5
- w_out: bfloat16 [128, 128], replicated, may hold values from -0.5 to 0.5
Outputs:
- update: bfloat16 [192, 192, 128], P('row', 'col')
The draws below stay inside these ranges and needn't reach their ends.
All inputs are finite; a program needn't handle non-finite values.
Results may differ from the reference program's by a relative error of at most 0.0083.
Values may be sent and summed in bfloat16 or wider, within the bound.
A program may use at most 64 MiB of HBM per device.

```python
import jax
import jax.numpy as jnp
from jax import lax

CZ = 128
CH = 128
TILES = 12
RES = 192
TILE = 16


def with_ends(result, stream_key, least, largest):
    extent = result.shape
    spot = [jax.random.randint(jax.random.fold_in(stream_key, axis), (), 0, extent[axis]) for axis in range(len(extent))]
    result = result.at[tuple(spot)].set(least)
    longest = extent.index(max(extent))
    spot[longest] = (spot[longest] + 1) % extent[longest]
    return result.at[tuple(spot)].set(largest)


def block_scale(own_key, extent, cuts, low, largest):
    gain, own = 1.0, jax.random.fold_in(own_key, 6)
    for position, shards_of in cuts:
        steps = jnp.exp(jax.random.uniform(jax.random.fold_in(own, position), (shards_of,), jnp.float32, low / len(cuts), largest / len(cuts)))
        gain = gain * jnp.repeat(steps, extent[position] // shards_of).reshape([-1 if axis == position else 1 for axis in range(len(extent))])
    return gain


def normal_values(key, shape, scale, most, cuts=(), kind=jnp.bfloat16):
    entries = scale * jax.random.normal(key, shape, jnp.float32)
    if cuts:
        entries = entries * block_scale(key, shape, cuts, -0.22, 0.18)
    return jnp.clip(entries, -most, most).astype(kind)


def setup_inputs(seed: int = 0) -> dict:
    arg_keys = jax.random.split(jax.random.key(seed), 9)
    return {
        "pair_act": normal_values(arg_keys[0], (RES, RES, CZ), 1.0, 6.0, ((0, 16), (1, 2))),
        "tile_mask": with_ends((jax.random.randint(arg_keys[1], (TILES, TILES), 0, 4) < 3).astype(jnp.int32), jax.random.fold_in(arg_keys[1], 1), 0, 1),
        "w_left_gate": normal_values(arg_keys[2], (CZ, CH), CZ ** -0.5, 0.5),
        "w_left": normal_values(arg_keys[3], (CZ, CH), CZ ** -0.5, 0.5),
        "w_right_gate": normal_values(arg_keys[4], (CZ, CH), CZ ** -0.5, 0.5),
        "w_right": normal_values(arg_keys[5], (CZ, CH), CZ ** -0.5, 0.5),
        "w_out_gate": normal_values(arg_keys[6], (CZ, CZ), CZ ** -0.5, 0.5),
        "w_out": normal_values(arg_keys[7], (CH, CZ), CH ** -0.5, 0.5),
    }


group_width = 8

def norm_last(values):
    mean = lax.optimization_barrier(jnp.mean(values, axis=-1, keepdims=True))
    centred = values - mean
    spread = lax.optimization_barrier(jnp.mean(centred * centred, axis=-1, keepdims=True))
    return centred * lax.rsqrt(spread + 1e-05)

def grouped(weight):
    return weight.reshape(CZ, CH // group_width, group_width).transpose(1, 0, 2)

def reference(pair_act, tile_mask, w_left_gate, w_left, w_right_gate, w_right, w_out_gate, w_out):
    normed = norm_last(pair_act.astype(jnp.float32)).astype(jnp.bfloat16)
    normed_f = lax.optimization_barrier(normed).astype(jnp.float32)
    tile_ids = jnp.arange(RES, dtype=jnp.int32) // TILE
    hot = (tile_ids[:, None] == jnp.arange(TILES, dtype=jnp.int32)[None, :]).astype(jnp.float32)
    pair_mask = jnp.dot(jnp.dot(hot, tile_mask.astype(jnp.float32), preferred_element_type=jnp.float32), hot.T, preferred_element_type=jnp.float32)

    def channel_group(weights):
        left_gate, left_value, right_gate, right_value = weights
        left = jax.nn.sigmoid(jnp.einsum('ikd,de->eik', normed_f, left_gate.astype(jnp.float32)))
        left = (left * jnp.einsum('ikd,de->eik', normed_f, left_value.astype(jnp.float32)) * pair_mask[None]).astype(jnp.bfloat16)
        right = jax.nn.sigmoid(jnp.einsum('jkd,de->ejk', normed_f, right_gate.astype(jnp.float32)))
        right = (right * jnp.einsum('jkd,de->ejk', normed_f, right_value.astype(jnp.float32)) * pair_mask[None]).astype(jnp.bfloat16)
        left_f = lax.optimization_barrier(left).astype(jnp.float32)
        right_f = lax.optimization_barrier(right).astype(jnp.float32)
        return jnp.einsum('cik,cjk->cij', left_f, right_f).astype(jnp.bfloat16)
    triangle = lax.map(channel_group, (grouped(w_left_gate), grouped(w_left), grouped(w_right_gate), grouped(w_right)))
    triangle = triangle.reshape(CH, RES, RES)
    triangle_f = jnp.transpose(lax.optimization_barrier(triangle), (1, 2, 0)).astype(jnp.float32)
    scaled = norm_last(triangle_f).astype(jnp.bfloat16)
    scaled_f = lax.optimization_barrier(scaled).astype(jnp.float32)
    projected = jnp.einsum('ijc,ce->ije', scaled_f, w_out.astype(jnp.float32))
    gate = jax.nn.sigmoid(jnp.einsum('ijd,de->ije', normed_f, w_out_gate.astype(jnp.float32)))
    return (gate * projected).astype(jnp.bfloat16)
```

```python
import functools

import jax
import jax.numpy as jnp
from jax import lax
from jax.experimental import pallas as pl
from jax.experimental.pallas import tpu as pltpu
from jax.sharding import PartitionSpec as P

TILES = 12
GROUP = 8
MESH = pl.DeviceIdType.MESH


def norm_axis(values, axis):
    mean = jnp.mean(values, axis=axis, keepdims=True)
    centred = values - mean
    spread = jnp.mean(centred * centred, axis=axis, keepdims=True)
    return centred * lax.rsqrt(spread + 1e-05)


def place(flat, col_size):
    return (flat // col_size, flat % col_size)


def greet(flat, first, count, col_size):
    barrier = pltpu.get_barrier_semaphore()

    def signal(step, _):
        other = first + (flat - first + step) % count
        pl.semaphore_signal(barrier, inc=1, device_id=place(other, col_size), device_id_type=MESH)
        return 0

    lax.fori_loop(1, count, signal, 0)
    pl.semaphore_wait(barrier, count - 1)


def spread_kernel(
    sizes, left, right, left_all, right_all, own_sem, left_send, left_recv, right_send, right_recv
):
    row_size, col_size, groups = sizes
    devices = row_size * col_size
    flat = lax.axis_index("row") * col_size + lax.axis_index("col")
    member = flat % groups
    first = flat - member

    def chunk(source, group):
        return source.at[group]

    own_left = pltpu.make_async_copy(chunk(left, member), left_all.at[member], own_sem.at[0])
    own_right = pltpu.make_async_copy(chunk(right, member), right_all.at[flat], own_sem.at[1])
    own_left.start()
    own_right.start()
    greet(flat, 0, devices, col_size)

    def right_copy(step):
        to = (flat + step) % devices
        return pltpu.make_async_remote_copy(
            src_ref=chunk(right, to % groups),
            dst_ref=right_all.at[flat],
            send_sem=right_send.at[step],
            recv_sem=right_recv.at[step],
            device_id=place(to, col_size),
            device_id_type=MESH,
        )

    def left_copy(step):
        to = (member + step) % groups
        return pltpu.make_async_remote_copy(
            src_ref=chunk(left, to),
            dst_ref=left_all.at[member],
            send_sem=left_send.at[step],
            recv_sem=left_recv.at[step],
            device_id=place(first + to, col_size),
            device_id_type=MESH,
        )

    def start_right(step, _):
        right_copy(step).start()
        return 0

    def start_left(step, _):
        left_copy(step).start()
        return 0

    def wait_right(step, _):
        right_copy(step).wait()
        return 0

    def wait_left(step, _):
        left_copy(step).wait()
        return 0

    lax.fori_loop(1, devices, start_right, 0)
    lax.fori_loop(1, groups, start_left, 0)
    own_left.wait()
    own_right.wait()
    lax.fori_loop(1, groups, wait_left, 0)
    lax.fori_loop(1, devices, wait_right, 0)


def return_kernel(sizes, triangle, owned, own_sem, send, recv):
    row_size, col_size, groups = sizes
    flat = lax.axis_index("row") * col_size + lax.axis_index("col")
    member = flat % groups
    first = flat - member
    own = pltpu.make_async_copy(triangle.at[member], owned.at[member], own_sem)
    own.start()
    greet(flat, first, groups, col_size)

    def copy(step):
        to = (member + step) % groups
        return pltpu.make_async_remote_copy(
            src_ref=triangle.at[to],
            dst_ref=owned.at[member],
            send_sem=send.at[step],
            recv_sem=recv.at[step],
            device_id=place(first + to, col_size),
            device_id_type=MESH,
        )

    def start(step, _):
        copy(step).start()
        return 0

    def wait(step, _):
        copy(step).wait()
        return 0

    lax.fori_loop(1, groups, start, 0)
    own.wait()
    lax.fori_loop(1, groups, wait, 0)


def local(
    sizes, pair_act, tile_mask, w_left_gate, w_left, w_right_gate, w_right, w_out_gate, w_out
):
    row_size, col_size, groups = sizes
    devices = row_size * col_size
    block_rows = groups // col_size
    rows, cols, width = pair_act.shape
    residues = rows * row_size
    tile = residues // TILES
    normed = norm_axis(pair_act.astype(jnp.float32), 2).astype(jnp.bfloat16)
    tile_range = lax.iota(jnp.int32, TILES)
    row_ids = (lax.axis_index("row") * rows + lax.iota(jnp.int32, rows)) // tile
    col_ids = (lax.axis_index("col") * cols + lax.iota(jnp.int32, cols)) // tile
    row_hot = (row_ids[:, None] == tile_range[None, :]).astype(jnp.float32)
    col_hot = (col_ids[:, None] == tile_range[None, :]).astype(jnp.float32)
    pair_mask = jnp.dot(
        jnp.dot(row_hot, tile_mask.astype(jnp.float32), preferred_element_type=jnp.float32),
        col_hot.T,
        preferred_element_type=jnp.float32,
    )
    pairs = rows * cols
    flat_normed = normed.reshape(pairs, width)
    flat_mask = pair_mask.reshape(1, pairs)

    def project(weight):
        return jnp.einsum("pd,de->ep", flat_normed, weight, preferred_element_type=jnp.float32)

    def factor(gate, value):
        out = jax.nn.sigmoid(project(gate)) * project(value) * flat_mask
        return out.astype(jnp.bfloat16).reshape(groups, GROUP, pairs)

    left = factor(w_left_gate, w_left)
    right = factor(w_right_gate, w_right)
    anywhere = pl.BlockSpec(memory_space=pl.ANY)
    left_all, right_all = pl.pallas_call(
        functools.partial(spread_kernel, sizes),
        out_shape=(
            jax.ShapeDtypeStruct((groups, GROUP, pairs), jnp.bfloat16),
            jax.ShapeDtypeStruct((devices, GROUP, pairs), jnp.bfloat16),
        ),
        in_specs=[anywhere] * 2,
        out_specs=(anywhere, anywhere),
        scratch_shapes=[
            pltpu.SemaphoreType.DMA((2,)),
            pltpu.SemaphoreType.DMA((groups,)),
            pltpu.SemaphoreType.DMA((groups,)),
            pltpu.SemaphoreType.DMA((devices,)),
            pltpu.SemaphoreType.DMA((devices,)),
        ],
        compiler_params=pltpu.CompilerParams(collective_id=0, has_side_effects=True),
    )(left, right)
    left_rows = (
        left_all.reshape(block_rows, col_size, GROUP, rows, cols)
        .transpose(2, 0, 3, 1, 4)
        .reshape(GROUP, block_rows * rows, residues)
    )
    right_rows = (
        right_all.reshape(row_size, col_size, GROUP, rows, cols)
        .transpose(2, 0, 3, 1, 4)
        .reshape(GROUP, residues, residues)
    )
    triangle = jnp.einsum(
        "cik,cjk->cij", left_rows, right_rows, preferred_element_type=jnp.float32
    ).astype(jnp.bfloat16)
    triangle = (
        triangle.reshape(GROUP, block_rows, rows, col_size, cols)
        .transpose(1, 3, 0, 2, 4)
        .reshape(groups, GROUP, pairs)
    )
    owned = pl.pallas_call(
        functools.partial(return_kernel, sizes),
        out_shape=jax.ShapeDtypeStruct((groups, GROUP, pairs), jnp.bfloat16),
        in_specs=[anywhere],
        out_specs=anywhere,
        scratch_shapes=[
            pltpu.SemaphoreType.DMA,
            pltpu.SemaphoreType.DMA((groups,)),
            pltpu.SemaphoreType.DMA((groups,)),
        ],
        compiler_params=pltpu.CompilerParams(collective_id=1, has_side_effects=True),
    )(triangle)
    owned = owned.reshape(width, pairs)
    scaled = norm_axis(owned.astype(jnp.float32), 0).astype(jnp.bfloat16)
    projected = jnp.einsum("cp,ce->pe", scaled, w_out, preferred_element_type=jnp.float32)
    gate = jax.nn.sigmoid(
        jnp.einsum("pd,de->pe", flat_normed, w_out_gate, preferred_element_type=jnp.float32)
    )
    return (gate * projected).astype(jnp.bfloat16).reshape(rows, cols, width)


def solution(mesh):
    def whole(pair_act, tile_mask, *weights):
        groups = pair_act.shape[2] // GROUP
        sizes = (mesh.shape["row"], mesh.shape["col"], groups)
        return jax.shard_map(
            functools.partial(local, sizes),
            mesh=mesh,
            in_specs=(P("row", "col", None), P(), P(), P(), P(), P(), P(), P()),
            out_specs=P("row", "col", None),
            check_vma=False,
        )(pair_act, tile_mask, *weights)

    return whole
```

```python
import functools

import jax
import jax.numpy as jnp
from jax import lax
from jax.experimental import pallas as pl
from jax.experimental.pallas import tpu as pltpu
from jax.sharding import PartitionSpec as P

TILES = 12
GROUP = 8
MESH = pl.DeviceIdType.MESH


def norm_axis(values, axis):
    mean = jnp.mean(values, axis=axis, keepdims=True)
    centred = values - mean
    spread = jnp.mean(centred * centred, axis=axis, keepdims=True)
    return centred * lax.rsqrt(spread + 1e-05)


def place(flat, col_size):
    return (flat // col_size, flat % col_size)


def greet(flat, first, count, col_size):
    barrier = pltpu.get_barrier_semaphore()

    def signal(step, _):
        other = first + (flat - first + step) % count
        pl.semaphore_signal(barrier, inc=1, device_id=place(other, col_size), device_id_type=MESH)
        return 0

    lax.fori_loop(1, count, signal, 0)
    pl.semaphore_wait(barrier, count - 1)


def spread_kernel(
    sizes, left, right, left_all, right_all, own_sem, left_send, left_recv, right_send, right_recv
):
    row_size, col_size, groups = sizes
    devices = row_size * col_size
    flat = lax.axis_index("row") * col_size + lax.axis_index("col")
    member = flat % groups
    first = flat - member

    def chunk(source, group):
        return source.at[group]

    own_left = pltpu.make_async_copy(chunk(left, member), left_all.at[member], own_sem.at[0])
    own_right = pltpu.make_async_copy(chunk(right, member), right_all.at[flat], own_sem.at[1])
    own_left.start()
    own_right.start()
    greet(flat, 0, devices, col_size)

    def right_copy(step):
        to = (flat + step) % devices
        return pltpu.make_async_remote_copy(
            src_ref=chunk(right, to % groups),
            dst_ref=right_all.at[flat],
            send_sem=right_send.at[step],
            recv_sem=right_recv.at[step],
            device_id=place(to, col_size),
            device_id_type=MESH,
        )

    def left_copy(step):
        to = (member + step) % groups
        return pltpu.make_async_remote_copy(
            src_ref=chunk(left, to),
            dst_ref=left_all.at[member],
            send_sem=left_send.at[step],
            recv_sem=left_recv.at[step],
            device_id=place(first + to, col_size),
            device_id_type=MESH,
        )

    def start_right(step, _):
        right_copy(step).start()
        return 0

    def start_left(step, _):
        left_copy(step).start()
        return 0

    def wait_right(step, _):
        right_copy(step).wait()
        return 0

    def wait_left(step, _):
        left_copy(step).wait()
        return 0

    lax.fori_loop(1, devices, start_right, 0)
    lax.fori_loop(1, groups, start_left, 0)
    own_left.wait()
    own_right.wait()
    lax.fori_loop(1, groups, wait_left, 0)
    lax.fori_loop(1, devices, wait_right, 0)


def return_kernel(sizes, triangle, owned, own_sem, send, recv):
    row_size, col_size, groups = sizes
    flat = lax.axis_index("row") * col_size + lax.axis_index("col")
    member = flat % groups
    first = flat - member
    own = pltpu.make_async_copy(triangle.at[member], owned.at[member], own_sem)
    own.start()
    greet(flat, first, groups, col_size)

    def copy(step):
        to = (member + step) % groups
        return pltpu.make_async_remote_copy(
            src_ref=triangle.at[to],
            dst_ref=owned.at[member],
            send_sem=send.at[step],
            recv_sem=recv.at[step],
            device_id=place(first + to, col_size),
            device_id_type=MESH,
        )

    def start(step, _):
        copy(step).start()
        return 0

    def wait(step, _):
        copy(step).wait()
        return 0

    lax.fori_loop(1, groups, start, 0)
    own.wait()
    lax.fori_loop(1, groups, wait, 0)


def local(
    sizes, pair_act, tile_mask, w_left_gate, w_left, w_right_gate, w_right, w_out_gate, w_out
):
    row_size, col_size, groups = sizes
    devices = row_size * col_size
    block_rows = groups // col_size
    rows, cols, width = pair_act.shape
    residues = rows * row_size
    tile = residues // TILES
    normed = norm_axis(pair_act.astype(jnp.float32), 2).astype(jnp.bfloat16)
    tile_range = lax.iota(jnp.int32, TILES)
    row_ids = (lax.axis_index("row") * rows + lax.iota(jnp.int32, rows)) // tile
    col_ids = (lax.axis_index("col") * cols + lax.iota(jnp.int32, cols)) // tile
    row_hot = (row_ids[:, None] == tile_range[None, :]).astype(jnp.float32)
    col_hot = (col_ids[:, None] == tile_range[None, :]).astype(jnp.float32)
    pair_mask = jnp.dot(
        jnp.dot(row_hot, tile_mask.astype(jnp.float32), preferred_element_type=jnp.float32),
        col_hot.T,
        preferred_element_type=jnp.float32,
    )
    pairs = rows * cols
    flat_normed = normed.reshape(pairs, width)
    flat_mask = pair_mask.reshape(1, pairs)

    def project(weight):
        return jnp.einsum("pd,de->ep", flat_normed, weight, preferred_element_type=jnp.float32)

    def factor(gate, value):
        out = jax.nn.sigmoid(project(gate)) * project(value) * flat_mask
        return out.astype(jnp.bfloat16).reshape(groups, GROUP, pairs)

    left = factor(w_left_gate, w_left)
    right = factor(w_right_gate, w_right)
    anywhere = pl.BlockSpec(memory_space=pl.ANY)
    left_all, right_all = pl.pallas_call(
        functools.partial(spread_kernel, sizes),
        out_shape=(
            jax.ShapeDtypeStruct((groups, GROUP, pairs), jnp.bfloat16),
            jax.ShapeDtypeStruct((devices, GROUP, pairs), jnp.bfloat16),
        ),
        in_specs=[anywhere] * 2,
        out_specs=(anywhere, anywhere),
        scratch_shapes=[
            pltpu.SemaphoreType.DMA((2,)),
            pltpu.SemaphoreType.DMA((groups,)),
            pltpu.SemaphoreType.DMA((groups,)),
            pltpu.SemaphoreType.DMA((devices,)),
            pltpu.SemaphoreType.DMA((devices,)),
        ],
        compiler_params=pltpu.CompilerParams(collective_id=0, has_side_effects=True),
    )(left, right)
    left_rows = (
        left_all.reshape(block_rows, col_size, GROUP, rows, cols)
        .transpose(2, 0, 3, 1, 4)
        .reshape(GROUP, block_rows * rows, residues)
    )
    right_rows = (
        right_all.reshape(row_size, col_size, GROUP, rows, cols)
        .transpose(2, 0, 3, 1, 4)
        .reshape(GROUP, residues, residues)
    )
    triangle = jnp.einsum(
        "cik,cjk->cij", left_rows, right_rows, preferred_element_type=jnp.float32
    ).astype(jnp.bfloat16)
    triangle = (
        triangle.reshape(GROUP, block_rows, rows, col_size, cols)
        .transpose(1, 3, 0, 2, 4)
        .reshape(groups, GROUP, pairs)
    )
    owned = pl.pallas_call(
        functools.partial(return_kernel, sizes),
        out_shape=jax.ShapeDtypeStruct((groups, GROUP, pairs), jnp.bfloat16),
        in_specs=[anywhere],
        out_specs=anywhere,
        scratch_shapes=[
            pltpu.SemaphoreType.DMA,
            pltpu.SemaphoreType.DMA((groups,)),
            pltpu.SemaphoreType.DMA((groups,)),
        ],
        compiler_params=pltpu.CompilerParams(collective_id=1, has_side_effects=True),
    )(triangle)
    owned = owned.reshape(width, pairs)
    scaled = norm_axis(owned.astype(jnp.float32), 0).astype(jnp.bfloat16)
    projected = jnp.einsum("cp,ce->pe", scaled, w_out, preferred_element_type=jnp.float32)
    gate = jax.nn.sigmoid(
        jnp.einsum("pd,de->pe", flat_normed, w_out_gate, preferred_element_type=jnp.float32)
    )
    return (gate * projected).astype(jnp.bfloat16).reshape(rows, cols, width)


LANES = 128


def fused_kernel(
    sizes, shape, pair, tiles, w_left_gate, w_left, w_right_gate, w_right, w_out_gate, w_out, out,
    normed, gate, left, right, left_all, right_all, left_mat, right_mat, product, triangle, owned,
    left_send, left_recv, right_send, right_recv, back_send, back_recv,
):
    row_size, col_size, groups = sizes
    rows, cols, width = shape
    devices = row_size * col_size
    blocks = devices // groups
    block_rows = groups // col_size
    pairs = rows * cols
    tile = rows * row_size // TILES
    row, col = lax.axis_index("row"), lax.axis_index("col")
    flat = row * col_size + col
    member = flat % groups
    block = flat // groups
    first = block * groups

    barrier = pltpu.get_barrier_semaphore()

    def signal(step, _):
        pl.semaphore_signal(
            barrier, inc=1, device_id=place((flat + step) % devices, col_size), device_id_type=MESH
        )
        return 0

    lax.fori_loop(1, devices, signal, 0)

    values = pair[...].astype(jnp.float32)
    normed[...] = norm_axis(values, 1).astype(jnp.bfloat16)

    spot = lax.broadcasted_iota(jnp.int32, (1, pairs), 1)
    within = spot
    for line in range(1, rows):
        within = jnp.where(spot >= line * cols, spot - line * cols, within)
    tile_ids = lax.broadcasted_iota(jnp.int32, (TILES, pairs), 0)
    row_low = (tile_ids * tile - row * rows) * cols
    row_hot = ((spot >= row_low) & (spot < row_low + tile * cols)).astype(jnp.float32)
    col_low = tile_ids * tile - col * cols
    col_hot = ((within >= col_low) & (within < col_low + tile)).astype(jnp.float32)
    picked = jnp.dot(tiles[...].astype(jnp.float32).T, row_hot, preferred_element_type=jnp.float32)
    mask = jnp.sum(picked * col_hot, axis=0, keepdims=True)

    def project(weight):
        turned = weight[...].astype(jnp.float32).T.astype(jnp.bfloat16)
        return lax.dot_general(
            turned, normed[...], (((1,), (1,)), ((), ())), preferred_element_type=jnp.float32
        )

    def factor(gate_weight, weight, target):
        made = jax.nn.sigmoid(project(gate_weight)) * project(weight) * mask
        for group in range(groups):
            target[group] = made[group * GROUP : (group + 1) * GROUP].astype(jnp.bfloat16)

    def right_copy(ahead, step):
        to = (member + step) % groups
        return pltpu.make_async_remote_copy(
            src_ref=right.at[to],
            dst_ref=right_all.at[flat],
            send_sem=right_send.at[ahead * groups + step],
            recv_sem=right_recv.at[ahead * groups + step],
            device_id=place((block + ahead) % blocks * groups + to, col_size),
            device_id_type=MESH,
        )

    def member_copy(source, target, send, recv, step):
        to = (member + step) % groups
        return pltpu.make_async_remote_copy(
            src_ref=source.at[to],
            dst_ref=target.at[member],
            send_sem=send.at[step],
            recv_sem=recv.at[step],
            device_id=place(first + to, col_size),
            device_id_type=MESH,
        )

    def left_copy(step):
        return member_copy(left, left_all, left_send, left_recv, step)

    def back_copy(step):
        return member_copy(triangle, owned, back_send, back_recv, step)

    def each(start, stop, do):
        def body(step, _):
            do(step)
            return 0

        lax.fori_loop(start, stop, body, 0)

    factor(w_right_gate, w_right, right)
    pl.semaphore_wait(barrier, devices - 1)
    for ahead in range(1, blocks):
        each(0, groups, lambda step: right_copy(ahead, step).start())
    each(1, groups, lambda step: right_copy(0, step).start())
    factor(w_left_gate, w_left, left)
    each(1, groups, lambda step: left_copy(step).start())

    gate[...] = jax.nn.sigmoid(
        jnp.dot(normed[...], w_out_gate[...], preferred_element_type=jnp.float32)
    )
    left_mat[...] = jnp.zeros_like(left_mat)
    right_mat[...] = jnp.zeros_like(right_mat)
    lane = lax.broadcasted_iota(jnp.int32, (GROUP, LANES), 1)

    def spread(chunk, target, half, start):
        parts = [
            chunk[:, at : at + LANES].astype(jnp.float32) for at in range(0, pairs, LANES)
        ]
        for line in range(rows):
            at, off = divmod(line * cols, LANES)
            part = parts[at]
            if off:
                part = pltpu.roll(part, LANES - off, 1)
                if off + cols > LANES:
                    part = jnp.where(
                        lane < LANES - off, part, pltpu.roll(parts[at + 1], LANES - off, 1)
                    )
            part = jnp.where(lane < cols, part, 0.0)
            target[half, pl.ds(pl.multiple_of((start + line) * GROUP, GROUP), GROUP), :] = part

    def place_right(source, chunk):
        line = source // col_size * rows
        start = line // cols * LANES + line % cols
        spread(chunk, right_mat, source % col_size, start)

    def place_left(source, chunk):
        spread(chunk, left_mat, source % col_size, source // col_size * rows)

    place_right(flat, right[member])
    place_left(member, left[member])

    def take_right(ahead, step):
        right_copy(ahead, step).wait_recv()
        source = (block - ahead + blocks) % blocks * groups + (member - step + groups) % groups
        place_right(source, right_all[source])

    def take_left(step):
        left_copy(step).wait_recv()
        source = (member - step + groups) % groups
        place_left(source, left_all[source])

    each(1, groups, lambda step: take_right(0, step))
    each(1, groups, take_left)
    for ahead in range(1, blocks):
        each(0, groups, lambda step: take_right(ahead, step))

    block_lines = block_rows * rows

    def channel(target, index, count):
        return jnp.concatenate(
            [
                target[half, pl.ds(index, count, stride=GROUP), :].astype(jnp.bfloat16)
                for half in range(col_size)
            ],
            axis=1,
        )

    for index in range(GROUP):
        made = lax.dot_general(
            channel(left_mat, index, block_lines),
            channel(right_mat, index, col_size * LANES),
            (((1,), (1,)), ((), ())),
            preferred_element_type=jnp.float32,
        )
        for half in range(col_size):
            product[half, pl.ds(index, block_lines, stride=GROUP), :] = made[
                :, half * LANES : (half + 1) * LANES
            ]

    def pack(to):
        half = to % col_size
        start = to // col_size * rows
        lines = [
            product[half, pl.ds(pl.multiple_of((start + line) * GROUP, GROUP), GROUP), :]
            for line in range(rows)
        ]
        for at in range(pairs // LANES):
            low = at * LANES
            line, off = divmod(low, cols)
            part = pltpu.roll(lines[line], LANES - off, 1) if off else lines[line]
            have = cols - off
            while have < LANES:
                line += 1
                following = pltpu.roll(lines[line], have, 1)
                part = jnp.where(lane < have, part, following)
                have += cols
            triangle[to, :, low : low + LANES] = part.astype(jnp.bfloat16)

    each(0, groups, pack)
    each(1, groups, lambda step: back_copy(step).start())
    owned[member] = triangle[member]
    each(1, groups, lambda step: left_copy(step).wait_send())
    each(1, groups, lambda step: right_copy(0, step).wait_send())
    for ahead in range(1, blocks):
        each(0, groups, lambda step: right_copy(ahead, step).wait_send())
    each(1, groups, lambda step: back_copy(step).wait())

    for at in range(0, pairs, LANES):
        piece = jnp.concatenate(
            [owned[group, :, at : at + LANES].astype(jnp.float32) for group in range(groups)],
            axis=0,
        )
        scaled = norm_axis(piece, 0).T.astype(jnp.bfloat16)
        projected = jnp.dot(scaled, w_out[...], preferred_element_type=jnp.float32)
        out[at : at + LANES] = (gate[at : at + LANES] * projected).astype(jnp.bfloat16)


def fused(sizes, pair_act, tile_mask, *weights):
    row_size, col_size, groups = sizes
    devices = row_size * col_size
    block_rows = groups // col_size
    rows, cols, width = pair_act.shape
    pairs = rows * cols
    kept = pl.BlockSpec(memory_space=pltpu.VMEM)
    dma = pltpu.SemaphoreType.DMA
    chunks = pltpu.VMEM((groups, GROUP, pairs), jnp.bfloat16)
    result = pl.pallas_call(
        functools.partial(fused_kernel, sizes, pair_act.shape),
        out_shape=jax.ShapeDtypeStruct((pairs, width), jnp.bfloat16),
        in_specs=[kept] * 8,
        out_specs=kept,
        scratch_shapes=[
            pltpu.VMEM((pairs, width), jnp.bfloat16),
            pltpu.VMEM((pairs, width), jnp.float32),
            chunks,
            chunks,
            chunks,
            pltpu.VMEM((devices, GROUP, pairs), jnp.bfloat16),
            pltpu.VMEM((col_size, block_rows * rows * GROUP, LANES), jnp.float32),
            pltpu.VMEM((col_size, col_size * LANES * GROUP, LANES), jnp.float32),
            pltpu.VMEM((col_size, block_rows * rows * GROUP, LANES), jnp.float32),
            chunks,
            chunks,
            dma((groups,)),
            dma((groups,)),
            dma((devices,)),
            dma((devices,)),
            dma((groups,)),
            dma((groups,)),
        ],
        compiler_params=pltpu.CompilerParams(collective_id=2, has_side_effects=True),
    )(pair_act.reshape(pairs, width), tile_mask, *weights)
    return result.reshape(rows, cols, width)


def fits(sizes, rows, cols):
    row_size, col_size, groups = sizes
    pairs = rows * cols
    return cols <= LANES and pairs % LANES == 0 and cols % rows == 0 and groups % col_size == 0


def solution(mesh):
    def whole(pair_act, tile_mask, *weights):
        groups = pair_act.shape[2] // GROUP
        sizes = (mesh.shape["row"], mesh.shape["col"], groups)
        rows, cols = (pair_act.shape[0] // sizes[0], pair_act.shape[1] // sizes[1])
        body = fused if fits(sizes, rows, cols) else local
        return jax.shard_map(
            functools.partial(body, sizes),
            mesh=mesh,
            in_specs=(P("row", "col", None), P(), P(), P(), P(), P(), P(), P()),
            out_specs=P("row", "col", None),
            check_vma=False,
        )(pair_act, tile_mask, *weights)

    return whole
```

```python
import functools

import jax
import jax.numpy as jnp
from jax import lax
from jax.experimental import pallas as pl
from jax.experimental.pallas import tpu as pltpu
from jax.sharding import PartitionSpec as P

TILES = 12
GROUP = 8
MESH = pl.DeviceIdType.MESH


def norm_axis(values, axis):
    mean = jnp.mean(values, axis=axis, keepdims=True)
    centred = values - mean
    spread = jnp.mean(centred * centred, axis=axis, keepdims=True)
    return centred * lax.rsqrt(spread + 1e-05)


def place(flat, col_size):
    return (flat // col_size, flat % col_size)


def greet(flat, first, count, col_size):
    barrier = pltpu.get_barrier_semaphore()

    def signal(step, _):
        other = first + (flat - first + step) % count
        pl.semaphore_signal(barrier, inc=1, device_id=place(other, col_size), device_id_type=MESH)
        return 0

    lax.fori_loop(1, count, signal, 0)
    pl.semaphore_wait(barrier, count - 1)


def spread_kernel(
    sizes, left, right, left_all, right_all, own_sem, left_send, left_recv, right_send, right_recv
):
    row_size, col_size, groups = sizes
    devices = row_size * col_size
    flat = lax.axis_index("row") * col_size + lax.axis_index("col")
    member = flat % groups
    first = flat - member

    def chunk(source, group):
        return source.at[group]

    own_left = pltpu.make_async_copy(chunk(left, member), left_all.at[member], own_sem.at[0])
    own_right = pltpu.make_async_copy(chunk(right, member), right_all.at[flat], own_sem.at[1])
    own_left.start()
    own_right.start()
    greet(flat, 0, devices, col_size)

    def right_copy(step):
        to = (flat + step) % devices
        return pltpu.make_async_remote_copy(
            src_ref=chunk(right, to % groups),
            dst_ref=right_all.at[flat],
            send_sem=right_send.at[step],
            recv_sem=right_recv.at[step],
            device_id=place(to, col_size),
            device_id_type=MESH,
        )

    def left_copy(step):
        to = (member + step) % groups
        return pltpu.make_async_remote_copy(
            src_ref=chunk(left, to),
            dst_ref=left_all.at[member],
            send_sem=left_send.at[step],
            recv_sem=left_recv.at[step],
            device_id=place(first + to, col_size),
            device_id_type=MESH,
        )

    def start_right(step, _):
        right_copy(step).start()
        return 0

    def start_left(step, _):
        left_copy(step).start()
        return 0

    def wait_right(step, _):
        right_copy(step).wait()
        return 0

    def wait_left(step, _):
        left_copy(step).wait()
        return 0

    lax.fori_loop(1, devices, start_right, 0)
    lax.fori_loop(1, groups, start_left, 0)
    own_left.wait()
    own_right.wait()
    lax.fori_loop(1, groups, wait_left, 0)
    lax.fori_loop(1, devices, wait_right, 0)


def return_kernel(sizes, triangle, owned, own_sem, send, recv):
    row_size, col_size, groups = sizes
    flat = lax.axis_index("row") * col_size + lax.axis_index("col")
    member = flat % groups
    first = flat - member
    own = pltpu.make_async_copy(triangle.at[member], owned.at[member], own_sem)
    own.start()
    greet(flat, first, groups, col_size)

    def copy(step):
        to = (member + step) % groups
        return pltpu.make_async_remote_copy(
            src_ref=triangle.at[to],
            dst_ref=owned.at[member],
            send_sem=send.at[step],
            recv_sem=recv.at[step],
            device_id=place(first + to, col_size),
            device_id_type=MESH,
        )

    def start(step, _):
        copy(step).start()
        return 0

    def wait(step, _):
        copy(step).wait()
        return 0

    lax.fori_loop(1, groups, start, 0)
    own.wait()
    lax.fori_loop(1, groups, wait, 0)


def local(
    sizes, pair_act, tile_mask, w_left_gate, w_left, w_right_gate, w_right, w_out_gate, w_out
):
    row_size, col_size, groups = sizes
    devices = row_size * col_size
    block_rows = groups // col_size
    rows, cols, width = pair_act.shape
    residues = rows * row_size
    tile = residues // TILES
    normed = norm_axis(pair_act.astype(jnp.float32), 2).astype(jnp.bfloat16)
    tile_range = lax.iota(jnp.int32, TILES)
    row_ids = (lax.axis_index("row") * rows + lax.iota(jnp.int32, rows)) // tile
    col_ids = (lax.axis_index("col") * cols + lax.iota(jnp.int32, cols)) // tile
    row_hot = (row_ids[:, None] == tile_range[None, :]).astype(jnp.float32)
    col_hot = (col_ids[:, None] == tile_range[None, :]).astype(jnp.float32)
    pair_mask = jnp.dot(
        jnp.dot(row_hot, tile_mask.astype(jnp.float32), preferred_element_type=jnp.float32),
        col_hot.T,
        preferred_element_type=jnp.float32,
    )
    pairs = rows * cols
    flat_normed = normed.reshape(pairs, width)
    flat_mask = pair_mask.reshape(1, pairs)

    def project(weight):
        return jnp.einsum("pd,de->ep", flat_normed, weight, preferred_element_type=jnp.float32)

    def factor(gate, value):
        out = jax.nn.sigmoid(project(gate)) * project(value) * flat_mask
        return out.astype(jnp.bfloat16).reshape(groups, GROUP, pairs)

    left = factor(w_left_gate, w_left)
    right = factor(w_right_gate, w_right)
    anywhere = pl.BlockSpec(memory_space=pl.ANY)
    left_all, right_all = pl.pallas_call(
        functools.partial(spread_kernel, sizes),
        out_shape=(
            jax.ShapeDtypeStruct((groups, GROUP, pairs), jnp.bfloat16),
            jax.ShapeDtypeStruct((devices, GROUP, pairs), jnp.bfloat16),
        ),
        in_specs=[anywhere] * 2,
        out_specs=(anywhere, anywhere),
        scratch_shapes=[
            pltpu.SemaphoreType.DMA((2,)),
            pltpu.SemaphoreType.DMA((groups,)),
            pltpu.SemaphoreType.DMA((groups,)),
            pltpu.SemaphoreType.DMA((devices,)),
            pltpu.SemaphoreType.DMA((devices,)),
        ],
        compiler_params=pltpu.CompilerParams(collective_id=0, has_side_effects=True),
    )(left, right)
    left_rows = (
        left_all.reshape(block_rows, col_size, GROUP, rows, cols)
        .transpose(2, 0, 3, 1, 4)
        .reshape(GROUP, block_rows * rows, residues)
    )
    right_rows = (
        right_all.reshape(row_size, col_size, GROUP, rows, cols)
        .transpose(2, 0, 3, 1, 4)
        .reshape(GROUP, residues, residues)
    )
    triangle = jnp.einsum(
        "cik,cjk->cij", left_rows, right_rows, preferred_element_type=jnp.float32
    ).astype(jnp.bfloat16)
    triangle = (
        triangle.reshape(GROUP, block_rows, rows, col_size, cols)
        .transpose(1, 3, 0, 2, 4)
        .reshape(groups, GROUP, pairs)
    )
    owned = pl.pallas_call(
        functools.partial(return_kernel, sizes),
        out_shape=jax.ShapeDtypeStruct((groups, GROUP, pairs), jnp.bfloat16),
        in_specs=[anywhere],
        out_specs=anywhere,
        scratch_shapes=[
            pltpu.SemaphoreType.DMA,
            pltpu.SemaphoreType.DMA((groups,)),
            pltpu.SemaphoreType.DMA((groups,)),
        ],
        compiler_params=pltpu.CompilerParams(collective_id=1, has_side_effects=True),
    )(triangle)
    owned = owned.reshape(width, pairs)
    scaled = norm_axis(owned.astype(jnp.float32), 0).astype(jnp.bfloat16)
    projected = jnp.einsum("cp,ce->pe", scaled, w_out, preferred_element_type=jnp.float32)
    gate = jax.nn.sigmoid(
        jnp.einsum("pd,de->pe", flat_normed, w_out_gate, preferred_element_type=jnp.float32)
    )
    return (gate * projected).astype(jnp.bfloat16).reshape(rows, cols, width)


LANES = 128


def fused_kernel(
    sizes, shape, pair_in, tiles_in, *rest
):
    weights_in, out = rest[:6], rest[6]
    (
        pair, tiles, w_left_gate, w_left, w_right_gate, w_right, w_out_gate, w_out, input_sem,
        normed, gate, left, right, left_all, right_all, left_mat, right_mat, left_lines, product, triangle, owned,
        left_send, left_recv, right_send, right_recv, back_send, back_recv,
    ) = rest[7:]
    kept = (pair, tiles, w_left_gate, w_left, w_right_gate, w_right, w_out_gate, w_out)
    fetches = [
        pltpu.make_async_copy(source, target, input_sem.at[index])
        for index, (source, target) in enumerate(zip((pair_in, tiles_in, *weights_in), kept))
    ]
    row_size, col_size, groups = sizes
    rows, cols, width = shape
    devices = row_size * col_size
    blocks = devices // groups
    block_rows = groups // col_size
    pairs = rows * cols
    tile = rows * row_size // TILES
    row, col = lax.axis_index("row"), lax.axis_index("col")
    flat = row * col_size + col
    member = flat % groups
    block = flat // groups
    first = block * groups

    barrier = pltpu.get_barrier_semaphore()

    def signal(step, _):
        pl.semaphore_signal(
            barrier, inc=1, device_id=place((flat + step) % devices, col_size), device_id_type=MESH
        )
        return 0

    fetches[0].start()
    lax.fori_loop(1, devices, signal, 0)
    for fetch in fetches[1:]:
        fetch.start()
    fetches[0].wait()

    values = pair[...].astype(jnp.float32)
    normed[...] = norm_axis(values, 1).astype(jnp.bfloat16)

    for fetch in fetches[1:]:
        fetch.wait()
    spot = lax.broadcasted_iota(jnp.int32, (1, pairs), 1)
    within = spot
    for line in range(1, rows):
        within = jnp.where(spot >= line * cols, spot - line * cols, within)
    tile_ids = lax.broadcasted_iota(jnp.int32, (TILES, pairs), 0)
    row_low = (tile_ids * tile - row * rows) * cols
    row_hot = ((spot >= row_low) & (spot < row_low + tile * cols)).astype(jnp.float32)
    col_low = tile_ids * tile - col * cols
    col_hot = ((within >= col_low) & (within < col_low + tile)).astype(jnp.float32)
    picked = jnp.dot(tiles[...].astype(jnp.float32).T, row_hot, preferred_element_type=jnp.float32)
    mask = jnp.sum(picked * col_hot, axis=0, keepdims=True)

    def project(weight):
        turned = weight[...].astype(jnp.float32).T.astype(jnp.bfloat16)
        return lax.dot_general(
            turned, normed[...], (((1,), (1,)), ((), ())), preferred_element_type=jnp.float32
        )

    def factor(gate_weight, weight, target):
        made = jax.nn.sigmoid(project(gate_weight)) * project(weight) * mask
        for group in range(groups):
            target[group] = made[group * GROUP : (group + 1) * GROUP].astype(jnp.bfloat16)

    def right_copy(ahead, step):
        to = (member + step) % groups
        return pltpu.make_async_remote_copy(
            src_ref=right.at[to],
            dst_ref=right_all.at[flat],
            send_sem=right_send.at[ahead * groups + step],
            recv_sem=right_recv.at[ahead * groups + step],
            device_id=place((block + ahead) % blocks * groups + to, col_size),
            device_id_type=MESH,
        )

    def member_copy(source, target, send, recv, step):
        to = (member + step) % groups
        return pltpu.make_async_remote_copy(
            src_ref=source.at[to],
            dst_ref=target.at[member],
            send_sem=send.at[step],
            recv_sem=recv.at[step],
            device_id=place(first + to, col_size),
            device_id_type=MESH,
        )

    def left_copy(step):
        return member_copy(left, left_all, left_send, left_recv, step)

    def back_copy(to, slot):
        return pltpu.make_async_remote_copy(
            src_ref=triangle.at[to],
            dst_ref=owned.at[slot],
            send_sem=back_send.at[to],
            recv_sem=back_recv.at[slot],
            device_id=place(first + to, col_size),
            device_id_type=MESH,
        )

    def each(start, stop, do):
        def body(step, _):
            do(step)
            return 0

        lax.fori_loop(start, stop, body, 0)

    factor(w_right_gate, w_right, right)
    factor(w_left_gate, w_left, left)
    pl.semaphore_wait(barrier, devices - 1)
    each(1, groups, lambda step: right_copy(0, step).start())
    each(1, groups, lambda step: left_copy(step).start())
    for ahead in range(1, blocks):
        each(0, groups, lambda step: right_copy(ahead, step).start())

    gate[...] = jax.nn.sigmoid(
        jnp.dot(normed[...], w_out_gate[...], preferred_element_type=jnp.float32)
    )
    left_mat[...] = jnp.zeros_like(left_mat)
    right_mat[...] = jnp.zeros_like(right_mat)
    lane = lax.broadcasted_iota(jnp.int32, (GROUP, LANES), 1)

    def spread(chunk, target, half, start):
        parts = [
            chunk[:, at : at + LANES].astype(jnp.float32) for at in range(0, pairs, LANES)
        ]
        for line in range(rows):
            at, off = divmod(line * cols, LANES)
            part = parts[at]
            if off:
                part = pltpu.roll(part, LANES - off, 1)
                if off + cols > LANES:
                    part = jnp.where(
                        lane < LANES - off, part, pltpu.roll(parts[at + 1], LANES - off, 1)
                    )
            part = jnp.where(lane < cols, part, 0.0)
            target[half, pl.ds(pl.multiple_of((start + line) * GROUP, GROUP), GROUP), :] = part

    def place_right(source, chunk):
        line = source // col_size * rows
        start = line // cols * LANES + line % cols
        spread(chunk, right_mat, source % col_size, start)

    def place_left(source, chunk):
        spread(chunk, left_mat, source % col_size, source // col_size * rows)

    place_right(flat, right[member])
    place_left(member, left[member])

    def take_right(ahead, step):
        right_copy(ahead, step).wait_recv()
        source = (block - ahead + blocks) % blocks * groups + (member - step + groups) % groups
        place_right(source, right_all[source])

    def take_left(step):
        left_copy(step).wait_recv()
        source = (member - step + groups) % groups
        place_left(source, left_all[source])

    each(1, groups, lambda step: take_right(0, step))
    each(1, groups, take_left)
    block_lines = block_rows * rows

    def channel(target, index, start, count):
        first_line = pl.multiple_of(start * GROUP, GROUP) + index
        return jnp.concatenate(
            [
                target[half, pl.ds(first_line, count, stride=GROUP), :].astype(jnp.bfloat16)
                for half in range(col_size)
            ],
            axis=1,
        )

    for index in range(GROUP):
        left_lines[index] = channel(left_mat, index, 0, block_lines)

    def finish(half):
        for index in range(GROUP):
            made = lax.dot_general(
                left_lines[index],
                channel(right_mat, index, half * LANES, LANES),
                (((1,), (1,)), ((), ())),
                preferred_element_type=jnp.float32,
            )
            product[pl.ds(index, block_lines, stride=GROUP), :] = made

        def pack(step):
            part_row = (member // col_size + step) % block_rows
            to = part_row * col_size + half
            lines = [
                product[pl.ds(pl.multiple_of((part_row * rows + line) * GROUP, GROUP), GROUP), :]
                for line in range(rows)
            ]
            for at in range(pairs // LANES):
                low = at * LANES
                line, off = divmod(low, cols)
                part = pltpu.roll(lines[line], LANES - off, 1) if off else lines[line]
                have = cols - off
                while have < LANES:
                    line += 1
                    part = jnp.where(lane < have, part, pltpu.roll(lines[line], have, 1))
                    have += cols
                triangle[to, :, low : low + LANES] = part.astype(jnp.bfloat16)

            @pl.when(to != member)
            def _():
                back_copy(to, member).start()

        each(0, block_rows, pack)

    finish(block)
    for ahead in range(1, blocks):
        each(0, groups, lambda step: take_right(ahead, step))
        finish((block - ahead + blocks) % blocks)
    owned[member] = triangle[member]
    each(1, groups, lambda step: left_copy(step).wait_send())
    each(1, groups, lambda step: right_copy(0, step).wait_send())
    for ahead in range(1, blocks):
        each(0, groups, lambda step: right_copy(ahead, step).wait_send())

    def wait_back(step):
        other = (member + step) % groups
        back_copy(other, other).wait()

    each(1, groups, wait_back)

    for at in range(0, pairs, LANES):
        piece = jnp.concatenate(
            [owned[group, :, at : at + LANES].astype(jnp.float32) for group in range(groups)],
            axis=0,
        )
        scaled = norm_axis(piece, 0).T.astype(jnp.bfloat16)
        projected = jnp.dot(scaled, w_out[...], preferred_element_type=jnp.float32)
        out[at : at + LANES] = (gate[at : at + LANES] * projected).astype(jnp.bfloat16)


def fused(sizes, pair_act, tile_mask, *weights):
    row_size, col_size, groups = sizes
    devices = row_size * col_size
    block_rows = groups // col_size
    rows, cols, width = pair_act.shape
    pairs = rows * cols
    kept = pl.BlockSpec(memory_space=pltpu.VMEM)
    dma = pltpu.SemaphoreType.DMA
    chunks = pltpu.VMEM((groups, GROUP, pairs), jnp.bfloat16)
    result = pl.pallas_call(
        functools.partial(fused_kernel, sizes, pair_act.shape),
        out_shape=jax.ShapeDtypeStruct((pairs, width), jnp.bfloat16),
        in_specs=[pl.BlockSpec(memory_space=pltpu.HBM)] * 8,
        out_specs=kept,
        scratch_shapes=[
            pltpu.VMEM((pairs, width), jnp.bfloat16),
            pltpu.VMEM(tile_mask.shape, tile_mask.dtype),
            *[pltpu.VMEM(weight.shape, weight.dtype) for weight in weights],
            dma((8,)),
            pltpu.VMEM((pairs, width), jnp.bfloat16),
            pltpu.VMEM((pairs, width), jnp.float32),
            chunks,
            chunks,
            chunks,
            pltpu.VMEM((devices, GROUP, pairs), jnp.bfloat16),
            pltpu.VMEM((col_size, block_rows * rows * GROUP, LANES), jnp.float32),
            pltpu.VMEM((col_size, col_size * LANES * GROUP, LANES), jnp.float32),
            pltpu.VMEM((GROUP, block_rows * rows, col_size * LANES), jnp.bfloat16),
            pltpu.VMEM((block_rows * rows * GROUP, LANES), jnp.float32),
            chunks,
            chunks,
            dma((groups,)),
            dma((groups,)),
            dma((devices,)),
            dma((devices,)),
            dma((groups,)),
            dma((groups,)),
        ],
        compiler_params=pltpu.CompilerParams(collective_id=2, has_side_effects=True),
    )(pair_act.reshape(pairs, width), tile_mask, *weights)
    return result.reshape(rows, cols, width)


def fits(sizes, rows, cols):
    row_size, col_size, groups = sizes
    pairs = rows * cols
    if row_size * col_size != groups * col_size or groups % col_size:
        return False
    return cols <= LANES and pairs % LANES == 0 and cols % rows == 0


def solution(mesh):
    def whole(pair_act, tile_mask, *weights):
        groups = pair_act.shape[2] // GROUP
        sizes = (mesh.shape["row"], mesh.shape["col"], groups)
        rows, cols = (pair_act.shape[0] // sizes[0], pair_act.shape[1] // sizes[1])
        body = fused if fits(sizes, rows, cols) else local
        return jax.shard_map(
            functools.partial(body, sizes),
            mesh=mesh,
            in_specs=(P("row", "col", None), P(), P(), P(), P(), P(), P(), P()),
            out_specs=P("row", "col", None),
            check_vma=False,
        )(pair_act, tile_mask, *weights)

    return whole
```

```python
import functools

import jax
import jax.numpy as jnp
from jax import lax
from jax.experimental import pallas as pl
from jax.experimental.pallas import tpu as pltpu
from jax.sharding import PartitionSpec as P

TILES = 12
GROUP = 8
MESH = pl.DeviceIdType.MESH


def norm_axis(values, axis):
    mean = jnp.mean(values, axis=axis, keepdims=True)
    centred = values - mean
    spread = jnp.mean(centred * centred, axis=axis, keepdims=True)
    return centred * lax.rsqrt(spread + 1e-05)


def place(flat, col_size):
    return (flat // col_size, flat % col_size)


def greet(flat, first, count, col_size):
    barrier = pltpu.get_barrier_semaphore()

    def signal(step, _):
        other = first + (flat - first + step) % count
        pl.semaphore_signal(barrier, inc=1, device_id=place(other, col_size), device_id_type=MESH)
        return 0

    lax.fori_loop(1, count, signal, 0)
    pl.semaphore_wait(barrier, count - 1)


def spread_kernel(
    sizes, left, right, left_all, right_all, own_sem, left_send, left_recv, right_send, right_recv
):
    row_size, col_size, groups = sizes
    devices = row_size * col_size
    flat = lax.axis_index("row") * col_size + lax.axis_index("col")
    member = flat % groups
    first = flat - member

    def chunk(source, group):
        return source.at[group]

    own_left = pltpu.make_async_copy(chunk(left, member), left_all.at[member], own_sem.at[0])
    own_right = pltpu.make_async_copy(chunk(right, member), right_all.at[flat], own_sem.at[1])
    own_left.start()
    own_right.start()
    greet(flat, 0, devices, col_size)

    def right_copy(step):
        to = (flat + step) % devices
        return pltpu.make_async_remote_copy(
            src_ref=chunk(right, to % groups),
            dst_ref=right_all.at[flat],
            send_sem=right_send.at[step],
            recv_sem=right_recv.at[step],
            device_id=place(to, col_size),
            device_id_type=MESH,
        )

    def left_copy(step):
        to = (member + step) % groups
        return pltpu.make_async_remote_copy(
            src_ref=chunk(left, to),
            dst_ref=left_all.at[member],
            send_sem=left_send.at[step],
            recv_sem=left_recv.at[step],
            device_id=place(first + to, col_size),
            device_id_type=MESH,
        )

    def start_right(step, _):
        right_copy(step).start()
        return 0

    def start_left(step, _):
        left_copy(step).start()
        return 0

    def wait_right(step, _):
        right_copy(step).wait()
        return 0

    def wait_left(step, _):
        left_copy(step).wait()
        return 0

    lax.fori_loop(1, devices, start_right, 0)
    lax.fori_loop(1, groups, start_left, 0)
    own_left.wait()
    own_right.wait()
    lax.fori_loop(1, groups, wait_left, 0)
    lax.fori_loop(1, devices, wait_right, 0)


def return_kernel(sizes, triangle, owned, own_sem, send, recv):
    row_size, col_size, groups = sizes
    flat = lax.axis_index("row") * col_size + lax.axis_index("col")
    member = flat % groups
    first = flat - member
    own = pltpu.make_async_copy(triangle.at[member], owned.at[member], own_sem)
    own.start()
    greet(flat, first, groups, col_size)

    def copy(step):
        to = (member + step) % groups
        return pltpu.make_async_remote_copy(
            src_ref=triangle.at[to],
            dst_ref=owned.at[member],
            send_sem=send.at[step],
            recv_sem=recv.at[step],
            device_id=place(first + to, col_size),
            device_id_type=MESH,
        )

    def start(step, _):
        copy(step).start()
        return 0

    def wait(step, _):
        copy(step).wait()
        return 0

    lax.fori_loop(1, groups, start, 0)
    own.wait()
    lax.fori_loop(1, groups, wait, 0)


def local(
    sizes, pair_act, tile_mask, w_left_gate, w_left, w_right_gate, w_right, w_out_gate, w_out
):
    row_size, col_size, groups = sizes
    devices = row_size * col_size
    block_rows = groups // col_size
    rows, cols, width = pair_act.shape
    residues = rows * row_size
    tile = residues // TILES
    normed = norm_axis(pair_act.astype(jnp.float32), 2).astype(jnp.bfloat16)
    tile_range = lax.iota(jnp.int32, TILES)
    row_ids = (lax.axis_index("row") * rows + lax.iota(jnp.int32, rows)) // tile
    col_ids = (lax.axis_index("col") * cols + lax.iota(jnp.int32, cols)) // tile
    row_hot = (row_ids[:, None] == tile_range[None, :]).astype(jnp.float32)
    col_hot = (col_ids[:, None] == tile_range[None, :]).astype(jnp.float32)
    pair_mask = jnp.dot(
        jnp.dot(row_hot, tile_mask.astype(jnp.float32), preferred_element_type=jnp.float32),
        col_hot.T,
        preferred_element_type=jnp.float32,
    )
    pairs = rows * cols
    flat_normed = normed.reshape(pairs, width)
    flat_mask = pair_mask.reshape(1, pairs)

    def project(weight):
        return jnp.einsum("pd,de->ep", flat_normed, weight, preferred_element_type=jnp.float32)

    def factor(gate, value):
        out = jax.nn.sigmoid(project(gate)) * project(value) * flat_mask
        return out.astype(jnp.bfloat16).reshape(groups, GROUP, pairs)

    left = factor(w_left_gate, w_left)
    right = factor(w_right_gate, w_right)
    anywhere = pl.BlockSpec(memory_space=pl.ANY)
    left_all, right_all = pl.pallas_call(
        functools.partial(spread_kernel, sizes),
        out_shape=(
            jax.ShapeDtypeStruct((groups, GROUP, pairs), jnp.bfloat16),
            jax.ShapeDtypeStruct((devices, GROUP, pairs), jnp.bfloat16),
        ),
        in_specs=[anywhere] * 2,
        out_specs=(anywhere, anywhere),
        scratch_shapes=[
            pltpu.SemaphoreType.DMA((2,)),
            pltpu.SemaphoreType.DMA((groups,)),
            pltpu.SemaphoreType.DMA((groups,)),
            pltpu.SemaphoreType.DMA((devices,)),
            pltpu.SemaphoreType.DMA((devices,)),
        ],
        compiler_params=pltpu.CompilerParams(collective_id=0, has_side_effects=True),
    )(left, right)
    left_rows = (
        left_all.reshape(block_rows, col_size, GROUP, rows, cols)
        .transpose(2, 0, 3, 1, 4)
        .reshape(GROUP, block_rows * rows, residues)
    )
    right_rows = (
        right_all.reshape(row_size, col_size, GROUP, rows, cols)
        .transpose(2, 0, 3, 1, 4)
        .reshape(GROUP, residues, residues)
    )
    triangle = jnp.einsum(
        "cik,cjk->cij", left_rows, right_rows, preferred_element_type=jnp.float32
    ).astype(jnp.bfloat16)
    triangle = (
        triangle.reshape(GROUP, block_rows, rows, col_size, cols)
        .transpose(1, 3, 0, 2, 4)
        .reshape(groups, GROUP, pairs)
    )
    owned = pl.pallas_call(
        functools.partial(return_kernel, sizes),
        out_shape=jax.ShapeDtypeStruct((groups, GROUP, pairs), jnp.bfloat16),
        in_specs=[anywhere],
        out_specs=anywhere,
        scratch_shapes=[
            pltpu.SemaphoreType.DMA,
            pltpu.SemaphoreType.DMA((groups,)),
            pltpu.SemaphoreType.DMA((groups,)),
        ],
        compiler_params=pltpu.CompilerParams(collective_id=1, has_side_effects=True),
    )(triangle)
    owned = owned.reshape(width, pairs)
    scaled = norm_axis(owned.astype(jnp.float32), 0).astype(jnp.bfloat16)
    projected = jnp.einsum("cp,ce->pe", scaled, w_out, preferred_element_type=jnp.float32)
    gate = jax.nn.sigmoid(
        jnp.einsum("pd,de->pe", flat_normed, w_out_gate, preferred_element_type=jnp.float32)
    )
    return (gate * projected).astype(jnp.bfloat16).reshape(rows, cols, width)


LANES = 128


def fused_kernel(
    sizes, shape, pair_in, tiles_in, *rest
):
    weights_in, out = rest[:6], rest[6]
    (
        pair, tiles, w_left_gate, w_left, w_right_gate, w_right, w_out_gate, w_out, input_sem, made_out, out_sem,
        normed, gate, left, right, left_all, right_all, left_mat, right_mat, left_lines, product, triangle, owned,
        left_send, left_recv, right_send, right_recv, back_send, back_recv,
    ) = rest[7:]
    kept = (pair, tiles, w_left_gate, w_left, w_right_gate, w_right, w_out_gate, w_out)
    fetches = [
        pltpu.make_async_copy(source, target, input_sem.at[index])
        for index, (source, target) in enumerate(zip((pair_in, tiles_in, *weights_in), kept))
    ]
    row_size, col_size, groups = sizes
    rows, cols, width = shape
    devices = row_size * col_size
    blocks = devices // groups
    block_rows = groups // col_size
    pairs = rows * cols
    tile = rows * row_size // TILES
    row, col = lax.axis_index("row"), lax.axis_index("col")
    flat = row * col_size + col
    member = flat % groups
    block = flat // groups
    first = block * groups

    barrier = pltpu.get_barrier_semaphore()

    def signal(step, _):
        pl.semaphore_signal(
            barrier, inc=1, device_id=place((flat + step) % devices, col_size), device_id_type=MESH
        )
        return 0

    fetches[0].start()
    lax.fori_loop(1, devices, signal, 0)
    for fetch in fetches[1:]:
        fetch.start()
    fetches[0].wait()

    values = pair[...].astype(jnp.float32)
    normed[...] = norm_axis(values, 1).astype(jnp.bfloat16)

    for fetch in fetches[1:]:
        fetch.wait()
    spot = lax.broadcasted_iota(jnp.int32, (1, pairs), 1)
    within = spot
    for line in range(1, rows):
        within = jnp.where(spot >= line * cols, spot - line * cols, within)
    tile_ids = lax.broadcasted_iota(jnp.int32, (TILES, pairs), 0)
    row_low = (tile_ids * tile - row * rows) * cols
    row_hot = ((spot >= row_low) & (spot < row_low + tile * cols)).astype(jnp.float32)
    col_low = tile_ids * tile - col * cols
    col_hot = ((within >= col_low) & (within < col_low + tile)).astype(jnp.float32)
    picked = jnp.dot(tiles[...].astype(jnp.float32).T, row_hot, preferred_element_type=jnp.float32)
    mask = jnp.sum(picked * col_hot, axis=0, keepdims=True)

    def project(weight):
        turned = weight[...].astype(jnp.float32).T.astype(jnp.bfloat16)
        return lax.dot_general(
            turned, normed[...], (((1,), (1,)), ((), ())), preferred_element_type=jnp.float32
        )

    def factor(gate_weight, weight, target):
        made = jax.nn.sigmoid(project(gate_weight)) * project(weight) * mask
        for group in range(groups):
            target[group] = made[group * GROUP : (group + 1) * GROUP].astype(jnp.bfloat16)

    def right_copy(ahead, step):
        to = (member + step) % groups
        return pltpu.make_async_remote_copy(
            src_ref=right.at[to],
            dst_ref=right_all.at[flat],
            send_sem=right_send.at[ahead * groups + step],
            recv_sem=right_recv.at[ahead * groups + step],
            device_id=place((block + ahead) % blocks * groups + to, col_size),
            device_id_type=MESH,
        )

    def member_copy(source, target, send, recv, step):
        to = (member + step) % groups
        return pltpu.make_async_remote_copy(
            src_ref=source.at[to],
            dst_ref=target.at[member],
            send_sem=send.at[step],
            recv_sem=recv.at[step],
            device_id=place(first + to, col_size),
            device_id_type=MESH,
        )

    def left_copy(step):
        return member_copy(left, left_all, left_send, left_recv, step)

    def back_copy(to, slot):
        return pltpu.make_async_remote_copy(
            src_ref=triangle.at[to],
            dst_ref=owned.at[slot],
            send_sem=back_send.at[to],
            recv_sem=back_recv.at[slot],
            device_id=place(first + to, col_size),
            device_id_type=MESH,
        )

    def each(start, stop, do):
        def body(step, _):
            do(step)
            return 0

        lax.fori_loop(start, stop, body, 0)

    factor(w_right_gate, w_right, right)
    factor(w_left_gate, w_left, left)
    pl.semaphore_wait(barrier, devices - 1)
    each(1, groups, lambda step: right_copy(0, step).start())
    each(1, groups, lambda step: left_copy(step).start())
    for ahead in range(1, blocks):
        each(0, groups, lambda step: right_copy(ahead, step).start())

    gate[...] = jax.nn.sigmoid(
        jnp.dot(normed[...], w_out_gate[...], preferred_element_type=jnp.float32)
    )
    left_mat[...] = jnp.zeros_like(left_mat)
    right_mat[...] = jnp.zeros_like(right_mat)
    lane = lax.broadcasted_iota(jnp.int32, (GROUP, LANES), 1)

    def spread(chunk, target, half, start):
        parts = [
            chunk[:, at : at + LANES].astype(jnp.float32) for at in range(0, pairs, LANES)
        ]
        for line in range(rows):
            at, off = divmod(line * cols, LANES)
            part = parts[at]
            if off:
                part = pltpu.roll(part, LANES - off, 1)
                if off + cols > LANES:
                    part = jnp.where(
                        lane < LANES - off, part, pltpu.roll(parts[at + 1], LANES - off, 1)
                    )
            part = jnp.where(lane < cols, part, 0.0)
            target[half, pl.ds(pl.multiple_of((start + line) * GROUP, GROUP), GROUP), :] = part

    def place_right(source, chunk):
        line = source // col_size * rows
        start = line // cols * LANES + line % cols
        spread(chunk, right_mat, source % col_size, start)

    def place_left(source, chunk):
        spread(chunk, left_mat, source % col_size, source // col_size * rows)

    place_right(flat, right[member])
    place_left(member, left[member])

    def take_right(ahead, step):
        right_copy(ahead, step).wait_recv()
        source = (block - ahead + blocks) % blocks * groups + (member - step + groups) % groups
        place_right(source, right_all[source])

    def take_left(step):
        left_copy(step).wait_recv()
        source = (member - step + groups) % groups
        place_left(source, left_all[source])

    each(1, groups, lambda step: take_right(0, step))
    each(1, groups, take_left)
    block_lines = block_rows * rows

    def channel(target, index, start, count):
        first_line = pl.multiple_of(start * GROUP, GROUP) + index
        return jnp.concatenate(
            [
                target[half, pl.ds(first_line, count, stride=GROUP), :].astype(jnp.bfloat16)
                for half in range(col_size)
            ],
            axis=1,
        )

    for index in range(GROUP):
        left_lines[index] = channel(left_mat, index, 0, block_lines)

    def finish(half):
        for index in range(GROUP):
            made = lax.dot_general(
                left_lines[index],
                channel(right_mat, index, half * LANES, LANES),
                (((1,), (1,)), ((), ())),
                preferred_element_type=jnp.float32,
            )
            product[pl.ds(index, block_lines, stride=GROUP), :] = made

        def pack(step):
            part_row = (member // col_size + step) % block_rows
            to = part_row * col_size + half
            lines = [
                product[pl.ds(pl.multiple_of((part_row * rows + line) * GROUP, GROUP), GROUP), :]
                for line in range(rows)
            ]
            for at in range(pairs // LANES):
                low = at * LANES
                line, off = divmod(low, cols)
                part = pltpu.roll(lines[line], LANES - off, 1) if off else lines[line]
                have = cols - off
                while have < LANES:
                    line += 1
                    part = jnp.where(lane < have, part, pltpu.roll(lines[line], have, 1))
                    have += cols
                triangle[to, :, low : low + LANES] = part.astype(jnp.bfloat16)

            @pl.when(to != member)
            def _():
                back_copy(to, member).start()

        each(0, block_rows, pack)

    finish(block)
    for ahead in range(1, blocks):
        each(0, groups, lambda step: take_right(ahead, step))
        finish((block - ahead + blocks) % blocks)
    owned[member] = triangle[member]
    each(1, groups, lambda step: left_copy(step).wait_send())
    each(1, groups, lambda step: right_copy(0, step).wait_send())
    for ahead in range(1, blocks):
        each(0, groups, lambda step: right_copy(ahead, step).wait_send())

    def wait_back(step):
        other = (member + step) % groups
        back_copy(other, other).wait()

    each(1, groups, wait_back)

    def hand_out(at):
        return pltpu.make_async_copy(
            made_out.at[pl.ds(at, LANES)], out.at[pl.ds(at, LANES)], out_sem.at[at // LANES]
        )

    for at in range(0, pairs, LANES):
        piece = jnp.concatenate(
            [owned[group, :, at : at + LANES].astype(jnp.float32) for group in range(groups)],
            axis=0,
        )
        scaled = norm_axis(piece, 0).T.astype(jnp.bfloat16)
        projected = jnp.dot(scaled, w_out[...], preferred_element_type=jnp.float32)
        made_out[at : at + LANES] = (gate[at : at + LANES] * projected).astype(jnp.bfloat16)
        hand_out(at).start()
    for at in range(0, pairs, LANES):
        hand_out(at).wait()


def fused(sizes, pair_act, tile_mask, *weights):
    row_size, col_size, groups = sizes
    devices = row_size * col_size
    block_rows = groups // col_size
    rows, cols, width = pair_act.shape
    pairs = rows * cols
    kept = pl.BlockSpec(memory_space=pltpu.VMEM)
    dma = pltpu.SemaphoreType.DMA
    chunks = pltpu.VMEM((groups, GROUP, pairs), jnp.bfloat16)
    result = pl.pallas_call(
        functools.partial(fused_kernel, sizes, pair_act.shape),
        out_shape=jax.ShapeDtypeStruct((pairs, width), jnp.bfloat16),
        in_specs=[pl.BlockSpec(memory_space=pltpu.HBM)] * 8,
        out_specs=pl.BlockSpec(memory_space=pltpu.HBM),
        scratch_shapes=[
            pltpu.VMEM((pairs, width), jnp.bfloat16),
            pltpu.VMEM(tile_mask.shape, tile_mask.dtype),
            *[pltpu.VMEM(weight.shape, weight.dtype) for weight in weights],
            dma((8,)),
            pltpu.VMEM((pairs, width), jnp.bfloat16),
            dma((pairs // LANES,)),
            pltpu.VMEM((pairs, width), jnp.bfloat16),
            pltpu.VMEM((pairs, width), jnp.float32),
            chunks,
            chunks,
            chunks,
            pltpu.VMEM((devices, GROUP, pairs), jnp.bfloat16),
            pltpu.VMEM((col_size, block_rows * rows * GROUP, LANES), jnp.float32),
            pltpu.VMEM((col_size, col_size * LANES * GROUP, LANES), jnp.float32),
            pltpu.VMEM((GROUP, block_rows * rows, col_size * LANES), jnp.bfloat16),
            pltpu.VMEM((block_rows * rows * GROUP, LANES), jnp.float32),
            chunks,
            chunks,
            dma((groups,)),
            dma((groups,)),
            dma((devices,)),
            dma((devices,)),
            dma((groups,)),
            dma((groups,)),
        ],
        compiler_params=pltpu.CompilerParams(collective_id=2, has_side_effects=True),
    )(pair_act.reshape(pairs, width), tile_mask, *weights)
    return result.reshape(rows, cols, width)


def fits(sizes, rows, cols):
    row_size, col_size, groups = sizes
    pairs = rows * cols
    if row_size * col_size != groups * col_size or groups % col_size:
        return False
    return cols <= LANES and pairs % LANES == 0 and cols % rows == 0


def solution(mesh):
    def whole(pair_act, tile_mask, *weights):
        groups = pair_act.shape[2] // GROUP
        sizes = (mesh.shape["row"], mesh.shape["col"], groups)
        rows, cols = (pair_act.shape[0] // sizes[0], pair_act.shape[1] // sizes[1])
        body = fused if fits(sizes, rows, cols) else local
        return jax.shard_map(
            functools.partial(body, sizes),
            mesh=mesh,
            in_specs=(P("row", "col", None), P(), P(), P(), P(), P(), P(), P()),
            out_specs=P("row", "col", None),
            check_vma=False,
        )(pair_act, tile_mask, *weights)

    return whole
```
